32 devices in a mesh: mode: 8 (over z, y), atom: 4 (over x, core).
Axes of the slice: x: 2, y: 2, z: 4, core: 2. Of those that a mesh axis runs over, the one named last changes fastest.
Arguments:
- vectors: bfloat16 [15360, 1024], P('atom', 'mode'), may hold values from -0.046875 to 0.046875
- couplings: float32 [4, 3, 3, 3, 5120], P(None, None, None, None, 'atom'), may hold values from -6 to 6, as said below
- neighbours: int32 [4, 5120], P(None, 'atom'), may hold values from 0 to 5119, as said below
- frequency: float32 [1024], replicated, may hold values from 1 to 2, as said below
Outputs:
- diffusivity: float32 [1024], P('mode')
The draws below stay inside these ranges and needn't reach their ends.
Inputs may be any that keep to these rules, and one draw needn't show every extreme that they name: neighbours[k, i] differs from i by 2 to 64 positions in atom order, counted around the end, upward for k < 2 and downward otherwise; the lists are mutual: neighbours[k + 2, neighbours[k, i]] = i for k < 2; some atoms in every slab have a neighbour exactly 64 positions above and some exactly 64 below. Antisymmetric bonds: couplings[k + 2, a, q, p, j] = -couplings[k, a, p, q, neighbours[k + 2, j]] for k < 2. `frequency`: strictly ascending.
All inputs are finite; a program needn't handle non-finite values.
Results may differ from the reference program's by a relative error of at most 0.00075.
Values may be sent and summed in bfloat16 or wider, within the bound.
A program may use at most 128 MiB of HBM per device.

```python
import math
import jax
import jax.numpy as jnp
from jax import lax

MODE_DEV = 128
ATOM_DEV = 1280
NEIGHBOURS = 4
HALO = 64
PARTNERS = 4
WIDTH_MODES = 320
BAND = 1024
ATOMS = 5120


def bond_table(key):
    half = NEIGHBOURS // 2
    window = HALO // 2
    offset_base = HALO - window + 1
    windows_all = ATOMS // window
    per_slab = ATOM_DEV // window
    atom_ids = jnp.arange(ATOMS, dtype=jnp.int32)
    window_ids = jnp.arange(windows_all, dtype=jnp.int32)[:, None]
    inner_ids = jnp.arange(window, dtype=jnp.int32)[None, :]
    upward_list = []
    downward_list = []
    for slot in range(half):
        scores = jax.random.randint(jax.random.fold_in(key, 31 + slot), (windows_all, window), 0, 1 << 20) * window + inner_ids
        forced = (window_ids % per_slab == 0) & (inner_ids == 0)
        scores = jnp.where(forced, (1 << 20) * window + window, scores).astype(jnp.int32)
        rank = jnp.argsort(jnp.argsort(scores, axis=1), axis=1).astype(jnp.int32).reshape(ATOMS)
        upward = jnp.mod(atom_ids + offset_base + rank - jnp.mod(atom_ids, window), ATOMS).astype(jnp.int32)
        downward = jnp.zeros((ATOMS,), jnp.int32).at[upward].set(atom_ids)
        upward_list.append(upward)
        downward_list.append(downward)
    return jnp.stack(upward_list + downward_list).astype(jnp.int32)


def draw_neighbours(key, part):
    return bond_table(key)


def draw_couplings(key, part):
    half = NEIGHBOURS // 2
    table = bond_table(key)
    base = jnp.clip(jax.random.normal(jax.random.fold_in(key, 41), (half, 3, 3, 3, ATOMS), jnp.float32), -6.0, 6.0)
    mirrored = []
    for slot in range(half):
        taken = jnp.take(base[slot], table[half + slot], axis=3)
        mirrored.append(-jnp.transpose(taken, (0, 2, 1, 3)))
    return jnp.concatenate([base, jnp.stack(mirrored)], axis=0).astype(jnp.float32)


def draw_frequency(key, part):
    gaps = jnp.exp(jax.random.uniform(jax.random.fold_in(key, 22), (BAND,), jnp.float32, jnp.log(0.25), 0.0))
    total = jnp.sum(gaps)
    position = (jnp.cumsum(gaps) - 0.5 * gaps) / total
    return (1.0 + position).astype(jnp.float32)


def shard_levels(key, shape, cuts, low, high):
    def one(axis_at, shards_of):
        steps = jax.random.uniform(jax.random.fold_in(jax.random.fold_in(key, 6), axis_at), (shards_of,), jnp.float32, low / len(cuts), high / len(cuts))
        return jnp.repeat(jnp.exp(steps), shape[axis_at] // shards_of).reshape((-1,) + (1,) * (len(shape) - axis_at - 1))

    gain = one(*cuts[0])
    for cut in cuts[1:]:
        gain = gain * one(*cut)
    return gain


def scatter_about(own_key, shape, scale, reach, split=(), held_as=jnp.bfloat16):
    level = shard_levels(own_key, shape, split, -0.22, 0.18) if split else 1.0
    drawn = jax.random.normal(own_key, shape, jnp.float32) * scale * level
    return jnp.minimum(jnp.maximum(drawn, -reach), reach).astype(held_as)


def setup_inputs(seed: int = 0) -> dict:
    keys = jax.random.split(jax.random.key(seed), 5)
    return {
        "vectors": scatter_about(keys[0], (3 * ATOMS, BAND), (3 * ATOMS) ** -0.5, 0.046875, ((0, 4), (1, 8))),
        "couplings": draw_couplings(jax.random.fold_in(keys[4], 71), 0),
        "neighbours": draw_neighbours(jax.random.fold_in(keys[4], 71), 0),
        "frequency": draw_frequency(jax.random.fold_in(keys[4], 71), 0),
    }


def velocity(padded, local_index, couplings):
    count = local_index.shape[1]
    block_width = padded.shape[2]
    coupled = jnp.transpose(couplings, (4, 0, 1, 2, 3))
    summed = jnp.zeros((count, 3, 3, block_width), jnp.float32)
    for slot in range(local_index.shape[0]):
        picked = jnp.take(padded, local_index[slot], axis=0).astype(jnp.float32)
        summed = summed + jnp.einsum("iapq,iqm->ipam", coupled[:, slot], picked)
    return summed.astype(jnp.bfloat16).reshape(count * 3, 3 * block_width)


def lorentz(offset, half_width):
    return (half_width / math.pi) / (offset * offset + half_width * half_width)


def weighted(cross_part, row_freq, col_freq, half_width):
    reshaped = cross_part.reshape(cross_part.shape[0], 3, -1)
    squares = jnp.sum(reshaped * reshaped, axis=1)
    return jnp.sum(squares * lorentz(row_freq[:, None] - col_freq[None, :], half_width), axis=1)


def reference(vectors, couplings, neighbours, frequency):
    blocks_all = BAND // MODE_DEV
    half_width = WIDTH_MODES / BAND
    rows_all = 3 * ATOMS
    stacked = vectors.reshape(ATOMS, 3, blocks_all, MODE_DEV).transpose(2, 0, 1, 3)
    applied = lax.map(lambda block_vectors: velocity(block_vectors, neighbours, couplings), stacked)
    flat = stacked.reshape(blocks_all, rows_all, MODE_DEV)
    vec_pad = jnp.concatenate([flat, jnp.zeros((PARTNERS, rows_all, MODE_DEV), flat.dtype)])
    app_pad = jnp.concatenate([applied, jnp.zeros((PARTNERS, rows_all, 3 * MODE_DEV), applied.dtype)])
    freq_pad = jnp.concatenate([frequency, jnp.ones((PARTNERS * MODE_DEV,), frequency.dtype)]).reshape(blocks_all + PARTNERS, MODE_DEV)

    def per_block(block_index):
        own_vec = lax.dynamic_index_in_dim(vec_pad, block_index, 0, keepdims=False)
        own_app = lax.dynamic_index_in_dim(app_pad, block_index, 0, keepdims=False)
        own_freq = lax.dynamic_index_in_dim(freq_pad, block_index, 0, keepdims=False)
        own_sum = weighted(jnp.dot(own_vec.T, own_app, preferred_element_type=jnp.float32), own_freq, own_freq, half_width)
        partner_list = []
        for distance in range(1, PARTNERS + 1):
            far_vec = lax.dynamic_index_in_dim(vec_pad, block_index + distance, 0, keepdims=False)
            far_app = lax.dynamic_index_in_dim(app_pad, block_index + distance, 0, keepdims=False)
            far_freq = lax.dynamic_index_in_dim(freq_pad, block_index + distance, 0, keepdims=False)
            own_sum = own_sum + weighted(jnp.dot(own_vec.T, far_app, preferred_element_type=jnp.float32), own_freq, far_freq, half_width)
            partner_list.append(weighted(jnp.dot(far_vec.T, own_app, preferred_element_type=jnp.float32), far_freq, own_freq, half_width))
        return own_sum, jnp.stack(partner_list)

    own_all, partner_all = lax.map(per_block, jnp.arange(blocks_all, dtype=jnp.int32))
    partner_pad = jnp.concatenate([jnp.zeros((PARTNERS, PARTNERS, MODE_DEV), jnp.float32), partner_all])
    for distance in range(1, PARTNERS + 1):
        own_all = own_all + partner_pad[PARTNERS - distance:PARTNERS - distance + blocks_all, distance - 1]
    freq_own = frequency.reshape(blocks_all, MODE_DEV)
    return (math.pi / (3.0 * freq_own * freq_own) * own_all).reshape(BAND)
```

```python
import functools
import math

import jax
import jax.numpy as jnp
from jax import lax
from jax.experimental import pallas as pl
from jax.experimental.pallas import tpu as pltpu
from jax.sharding import PartitionSpec as P

HALO = 64
PARTNERS = 4
WIDTH_MODES = 320
TILE = 128
LOWER_COMPUTES = {4: True, 3: False, 2: False, 1: True}


def passed_along(block, axis, distance):
    devices = range(lax.axis_size(axis))
    route = [(i - distance, i) for i in devices if i - distance in devices]
    return lax.ppermute(block, axis, route)


def rolled(block, axis, shift):
    count = lax.axis_size(axis)
    return lax.ppermute(block, axis, [(i, (i + shift) % count) for i in range(count)])


def velocity_kernel(rows_ref, index_ref, coupling_ref, out_ref, planes, split, merge, hot, weights):
    modes = rows_ref.shape[1]
    wide = 3 * TILE
    window = 2 * TILE
    tile = pl.program_id(0)

    @pl.when(tile == 0)
    def _():
        row = lax.broadcasted_iota(jnp.int32, (wide, wide), 0)
        col = lax.broadcasted_iota(jnp.int32, (wide, wide), 1)
        here = row == 3 * (col % TILE) + col // TILE
        split[...] = jnp.where(here, 1.0, 0.0).astype(jnp.bfloat16)
        there = col == 3 * (row % TILE) + row // TILE
        merge[...] = jnp.where(there, 1.0, 0.0).astype(jnp.bfloat16)

        def deinterleave(chunk, carry):
            source = rows_ref[pl.ds(pl.multiple_of(chunk * wide, wide), wide), :]
            moved = lax.dot_general(
                source, split[...], (((0,), (0,)), ((), ())), preferred_element_type=jnp.float32
            ).astype(jnp.bfloat16)
            for q in range(3):
                planes[q, :, pl.ds(pl.multiple_of(chunk * TILE, TILE), TILE)] = moved[
                    :, q * TILE : (q + 1) * TILE
                ]
            return carry

        lax.fori_loop(0, rows_ref.shape[0] // wide, deinterleave, 0)

    place = lax.broadcasted_iota(jnp.int32, (window, TILE), 0) + tile * TILE
    for slot in range(4):
        hot[slot] = jnp.where(place == index_ref[slot : slot + 1, :], 1.0, 0.0).astype(jnp.bfloat16)

    lanes = pl.ds(pl.multiple_of(tile * TILE, TILE), window)
    gathered = jnp.concatenate([planes[q, :, lanes] for q in range(3)], axis=1)
    reach = window - HALO

    def masked(slot, start, a, p, q):
        value = coupling_ref[slot, a, p, q : q + 1, :]
        packed = jnp.broadcast_to(value, (16, TILE)).astype(jnp.bfloat16)
        flags = hot[slot, start : start + reach, :].reshape(reach // 16, 16, TILE)
        return flags * packed[None]

    for a in range(3):
        for p in range(3):
            for q in range(3):
                up = masked(0, HALO, a, p, q) + masked(1, HALO, a, p, q)
                down = masked(2, 0, a, p, q) + masked(3, 0, a, p, q)
                edge = HALO // 16
                inner = up[: reach // 16 - edge] + down[edge:]
                full = jnp.concatenate([down[:edge], inner, up[reach // 16 - edge :]], axis=0)
                weights[q * window : (q + 1) * window, p * TILE : (p + 1) * TILE] = full.reshape(
                    window, TILE
                )
        applied = jnp.dot(gathered, weights[...], preferred_element_type=jnp.float32)
        native = jnp.dot(
            applied.astype(jnp.bfloat16), merge[...], preferred_element_type=jnp.float32
        )
        out_ref[a * modes : (a + 1) * modes, :] = native.astype(jnp.bfloat16)


def velocity(padded, local_index, couplings):
    atoms_dev = local_index.shape[1]
    modes = padded.shape[1]
    wide = 3 * TILE
    padded_atoms = padded.shape[0] // 3
    return pl.pallas_call(
        velocity_kernel,
        grid=(atoms_dev // TILE,),
        out_shape=jax.ShapeDtypeStruct((3 * modes, 3 * atoms_dev), jnp.bfloat16),
        in_specs=[
            pl.BlockSpec(padded.shape, lambda t: (0, 0)),
            pl.BlockSpec((4, TILE), lambda t: (0, t)),
            pl.BlockSpec((4, 3, 3, 3, TILE), lambda t: (0, 0, 0, 0, t)),
        ],
        out_specs=pl.BlockSpec((3 * modes, wide), lambda t: (0, t)),
        scratch_shapes=[
            pltpu.VMEM((3, modes, padded_atoms), jnp.bfloat16),
            pltpu.VMEM((wide, wide), jnp.bfloat16),
            pltpu.VMEM((wide, wide), jnp.bfloat16),
            pltpu.VMEM((4, 2 * TILE, TILE), jnp.bfloat16),
            pltpu.VMEM((6 * TILE, wide), jnp.bfloat16),
        ],
        compiler_params=pltpu.CompilerParams(
            dimension_semantics=("arbitrary",), vmem_limit_bytes=32 * 1024 * 1024
        ),
        cost_estimate=pl.CostEstimate(
            flops=54 * 2 * TILE * atoms_dev * modes * 4, bytes_accessed=6_000_000, transcendentals=0
        ),
        name="velocity",
    )(padded, local_index, couplings)


def lorentz(offset, half_width):
    return half_width / math.pi / (offset * offset + half_width * half_width)


def local(vectors, couplings, neighbours, frequency):
    rows_dev, block_width = vectors.shape
    atoms_dev = rows_dev // 3
    groups = lax.axis_size("atom")
    total_atoms = atoms_dev * groups
    atom_index = lax.axis_index("atom")
    first_atom = atom_index * atoms_dev
    local_index = jnp.mod(neighbours - first_atom + HALO, total_atoms)
    head = vectors[: 3 * HALO]
    tail = vectors[rows_dev - 3 * HALO :]
    padded = jnp.concatenate([rolled(tail, "atom", 1), vectors, rolled(head, "atom", -1)], axis=0)
    far = {}
    for distance in sorted(LOWER_COMPUTES, reverse=True):
        sign = -1 if LOWER_COMPUTES[distance] else 1
        far[distance] = passed_along(vectors, "mode", sign * distance)
    applied = velocity(padded, local_index, couplings)

    modes_all = block_width * lax.axis_size("mode")
    half_width = WIDTH_MODES / modes_all
    block_index = lax.axis_index("mode")
    part = block_width // groups

    def freq_of(block, first, width):
        return lax.dynamic_slice_in_dim(frequency, block * block_width + first, width)

    own_freq = freq_of(block_index, 0, block_width)
    part_freq = freq_of(block_index, atom_index * part, part)

    def summed(other):
        joint = jnp.dot(applied, other, preferred_element_type=jnp.float32)
        split = joint.astype(jnp.bfloat16).reshape(3, groups, part, block_width)

        def piece(owner):
            return lax.dynamic_index_in_dim(split, owner, 1, keepdims=False)

        total = piece(atom_index).astype(jnp.float32)
        for shift in range(1, groups):
            sent = piece(lax.rem(atom_index + shift, groups))
            total = total + rolled(sent, "atom", shift).astype(jnp.float32)
        return jnp.sum(total * total, axis=0)

    own_part = jnp.sum(
        summed(vectors) * lorentz(part_freq[:, None] - own_freq[None, :], half_width), axis=1
    )
    returned = jnp.zeros((block_width,), jnp.float32)
    for distance in (1, 2, 3, 4):
        sign = -1 if LOWER_COMPUTES[distance] else 1
        far_freq = freq_of(block_index - sign * distance, 0, block_width)
        terms = summed(far[distance]) * lorentz(part_freq[:, None] - far_freq[None, :], half_width)
        own_part = own_part + jnp.sum(terms, axis=1)
        returned = returned + passed_along(jnp.sum(terms, axis=0), "mode", -sign * distance)
    total = lax.dynamic_update_slice_in_dim(
        jnp.zeros((block_width,), jnp.float32), own_part, atom_index * part, 0
    )
    total = total + returned
    held = jnp.stack([total] + [rolled(total, "atom", shift) for shift in range(1, groups)])
    order = lax.rem(atom_index - jnp.arange(groups, dtype=jnp.int32) + groups, groups)
    result = jnp.zeros((block_width,), jnp.float32)
    for slab in range(groups):
        result = result + jnp.sum(jnp.where((order == slab)[:, None], held, 0.0), axis=0)
    return math.pi / (3.0 * own_freq * own_freq) * result


def solution(mesh):
    return jax.shard_map(
        local,
        mesh=mesh,
        in_specs=(P("atom", "mode"), P(None, None, None, None, "atom"), P(None, "atom"), P()),
        out_specs=P("mode"),
        check_vma=False,
    )
```

```python
import math

import jax
import jax.numpy as jnp
from jax import lax
from jax.experimental import pallas as pl
from jax.experimental.pallas import tpu as pltpu
from jax.sharding import PartitionSpec as P

HALO = 64
PARTNERS = 4
WIDTH_MODES = 320
TILE = 128
LOWER_COMPUTES = {2: True, 1: False, 3: False, 4: True}
BATCHES = ((0, 2, 1), (3, 4))


def passed_along(block, axis, distance):
    devices = range(lax.axis_size(axis))
    route = [(i - distance, i) for i in devices if i - distance in devices]
    return lax.ppermute(block, axis, route)


def rolled(block, axis, shift):
    count = lax.axis_size(axis)
    return lax.ppermute(block, axis, [(i, (i + shift) % count) for i in range(count)])


def velocity_kernel(rows_ref, index_ref, coupling_ref, out_ref, planes, split, merge, hot, weights):
    modes = rows_ref.shape[1]
    wide = 3 * TILE
    window = 2 * TILE
    tile = pl.program_id(0)

    @pl.when(tile == 0)
    def _():
        row = lax.broadcasted_iota(jnp.int32, (wide, wide), 0)
        col = lax.broadcasted_iota(jnp.int32, (wide, wide), 1)
        here = row == 3 * (col % TILE) + col // TILE
        split[...] = jnp.where(here, 1.0, 0.0).astype(jnp.bfloat16)
        there = col == 3 * (row % TILE) + row // TILE
        merge[...] = jnp.where(there, 1.0, 0.0).astype(jnp.bfloat16)

        def deinterleave(chunk, carry):
            source = rows_ref[pl.ds(pl.multiple_of(chunk * wide, wide), wide), :]
            moved = lax.dot_general(
                source, split[...], (((0,), (0,)), ((), ())), preferred_element_type=jnp.float32
            ).astype(jnp.bfloat16)
            for q in range(3):
                planes[q, :, pl.ds(pl.multiple_of(chunk * TILE, TILE), TILE)] = moved[
                    :, q * TILE : (q + 1) * TILE
                ]
            return carry

        lax.fori_loop(0, rows_ref.shape[0] // wide, deinterleave, 0)

    place = lax.broadcasted_iota(jnp.int32, (window, TILE), 0) + tile * TILE
    for slot in range(4):
        hot[slot] = jnp.where(place == index_ref[slot : slot + 1, :], 1.0, 0.0).astype(jnp.bfloat16)

    lanes = pl.ds(pl.multiple_of(tile * TILE, TILE), window)
    gathered = jnp.concatenate([planes[q, :, lanes] for q in range(3)], axis=1)
    reach = window - HALO

    def masked(slot, start, a, p, q):
        value = coupling_ref[slot, a, p, q : q + 1, :]
        packed = jnp.broadcast_to(value, (16, TILE)).astype(jnp.bfloat16)
        flags = hot[slot, start : start + reach, :].reshape(reach // 16, 16, TILE)
        return flags * packed[None]

    for a in range(3):
        for p in range(3):
            for q in range(3):
                up = masked(0, HALO, a, p, q) + masked(1, HALO, a, p, q)
                down = masked(2, 0, a, p, q) + masked(3, 0, a, p, q)
                edge = HALO // 16
                inner = up[: reach // 16 - edge] + down[edge:]
                full = jnp.concatenate([down[:edge], inner, up[reach // 16 - edge :]], axis=0)
                weights[q * window : (q + 1) * window, p * TILE : (p + 1) * TILE] = full.reshape(
                    window, TILE
                )
        applied = jnp.dot(gathered, weights[...], preferred_element_type=jnp.float32)
        native = jnp.dot(
            applied.astype(jnp.bfloat16), merge[...], preferred_element_type=jnp.float32
        )
        out_ref[a * modes : (a + 1) * modes, :] = native.astype(jnp.bfloat16)


def velocity(padded, local_index, couplings):
    atoms_dev = local_index.shape[1]
    modes = padded.shape[1]
    wide = 3 * TILE
    padded_atoms = padded.shape[0] // 3
    return pl.pallas_call(
        velocity_kernel,
        grid=(atoms_dev // TILE,),
        out_shape=jax.ShapeDtypeStruct((3 * modes, 3 * atoms_dev), jnp.bfloat16),
        in_specs=[
            pl.BlockSpec(padded.shape, lambda t: (0, 0)),
            pl.BlockSpec((4, TILE), lambda t: (0, t)),
            pl.BlockSpec((4, 3, 3, 3, TILE), lambda t: (0, 0, 0, 0, t)),
        ],
        out_specs=pl.BlockSpec((3 * modes, wide), lambda t: (0, t)),
        scratch_shapes=[
            pltpu.VMEM((3, modes, padded_atoms), jnp.bfloat16),
            pltpu.VMEM((wide, wide), jnp.bfloat16),
            pltpu.VMEM((wide, wide), jnp.bfloat16),
            pltpu.VMEM((4, 2 * TILE, TILE), jnp.bfloat16),
            pltpu.VMEM((6 * TILE, wide), jnp.bfloat16),
        ],
        compiler_params=pltpu.CompilerParams(
            dimension_semantics=("arbitrary",), vmem_limit_bytes=32 * 1024 * 1024
        ),
        cost_estimate=pl.CostEstimate(
            flops=54 * 2 * TILE * atoms_dev * modes * 4, bytes_accessed=6_000_000, transcendentals=0
        ),
        name="velocity",
    )(padded, local_index, couplings)


def lorentz(offset, half_width):
    return half_width / math.pi / (offset * offset + half_width * half_width)


def local(vectors, couplings, neighbours, frequency):
    rows_dev, block_width = vectors.shape
    atoms_dev = rows_dev // 3
    groups = lax.axis_size("atom")
    total_atoms = atoms_dev * groups
    atom_index = lax.axis_index("atom")
    first_atom = atom_index * atoms_dev
    local_index = jnp.mod(neighbours - first_atom + HALO, total_atoms)
    head = vectors[: 3 * HALO]
    tail = vectors[rows_dev - 3 * HALO :]
    padded = jnp.concatenate([rolled(tail, "atom", 1), vectors, rolled(head, "atom", -1)], axis=0)
    far = {}
    for distance in (2, 3, 1):
        sign = -1 if LOWER_COMPUTES[distance] else 1
        far[distance] = passed_along(vectors, "mode", sign * distance)
    far[4] = passed_along(far[2], "mode", -2)
    far[0] = vectors
    applied = velocity(padded, local_index, couplings)

    modes_all = block_width * lax.axis_size("mode")
    half_width = WIDTH_MODES / modes_all
    block_index = lax.axis_index("mode")
    part = block_width // groups

    def freq_of(block, first, width):
        return lax.dynamic_slice_in_dim(frequency, block * block_width + first, width)

    own_freq = freq_of(block_index, 0, block_width)
    part_freq = freq_of(block_index, atom_index * part, part)

    def summed(batch):
        split = jnp.stack(
            [
                jnp.dot(applied, far[distance], preferred_element_type=jnp.float32)
                .astype(jnp.bfloat16)
                .reshape(3, groups, part, block_width)
                for distance in batch
            ]
        )

        def piece(owner):
            return lax.dynamic_index_in_dim(split, owner, 2, keepdims=False)

        total = piece(atom_index).astype(jnp.float32)
        for shift in range(1, groups):
            sent = piece(lax.rem(atom_index + shift, groups))
            total = total + rolled(sent, "atom", shift).astype(jnp.float32)
        return jnp.sum(total * total, axis=1)

    own_part = jnp.zeros((part,), jnp.float32)
    returned = jnp.zeros((block_width,), jnp.float32)
    for batch in BATCHES:
        squares = summed(batch)
        for at, distance in enumerate(batch):
            sign = -1 if LOWER_COMPUTES.get(distance) else 1
            far_freq = freq_of(block_index - sign * distance, 0, block_width)
            terms = squares[at] * lorentz(part_freq[:, None] - far_freq[None, :], half_width)
            own_part = own_part + jnp.sum(terms, axis=1)
            if distance:
                returned = returned + passed_along(
                    jnp.sum(terms, axis=0), "mode", -sign * distance
                )
    total = lax.dynamic_update_slice_in_dim(
        jnp.zeros((block_width,), jnp.float32), own_part, atom_index * part, 0
    )
    total = total + returned
    held = jnp.stack([total] + [rolled(total, "atom", shift) for shift in range(1, groups)])
    order = lax.rem(atom_index - jnp.arange(groups, dtype=jnp.int32) + groups, groups)
    result = jnp.zeros((block_width,), jnp.float32)
    for slab in range(groups):
        result = result + jnp.sum(jnp.where((order == slab)[:, None], held, 0.0), axis=0)
    return math.pi / (3.0 * own_freq * own_freq) * result


def solution(mesh):
    return jax.shard_map(
        local,
        mesh=mesh,
        in_specs=(P("atom", "mode"), P(None, None, None, None, "atom"), P(None, "atom"), P()),
        out_specs=P("mode"),
        check_vma=False,
    )
```
